512 devices in a mesh: grp: 2 (over y), wide: 128 (over x, z), narrow: 2 (over core).
Axes of the slice: x: 4, y: 2, z: 32, core: 2. Of those that a mesh axis runs over, the one named last changes fastest.
The devices are a block of a 4x8x32 slice.
Arguments:
- cache: bfloat16 [256, 768, 576], P('grp', ('wide', 'narrow')), parts along dimension 0, may hold values from -4 to 4
- lengths: int32 [256], P('grp'), parts along dimension 0, may hold values from 1 to 767, 32768 in all
- slots: int32 [256], P('grp'), parts along dimension 0, may hold values from 0 to 127, each once
- query: bfloat16 [256, 1, 64, 576], P(('grp', 'wide'), None, 'narrow'), parts along dimension 0, may hold values from -200 to 200
Outputs:
- attended: bfloat16 [256, 1, 64, 512], P(('grp', 'wide'), None, 'narrow'), parts along dimension 0
The draws below stay inside these ranges and needn't reach their ends.
There are 2 independent parts, one for each index of `grp`. The reference program is written for one: setup_inputs(seed, part) draws one part's arguments, and reference() takes and returns one part's arrays. A program takes and returns all parts, laid end to end along the dimension named above; each array names one. Nothing has to cross between parts.
Inputs may be any that keep to these rules, and one draw needn't show every extreme that they name: `lengths`: each request has at most 767 cached positions, and some request has exactly that many in every draw; its 1 new tokens' entries follow its cached positions. `slots`: A permutation: every slot holds one request.
All inputs are finite; a program needn't handle non-finite values.
Results may differ from the reference program's by a relative error of at most 0.013.
Values may be sent and summed in bfloat16 or wider, within the bound.
No kernel may reach another device: no remote copies, remote signals or barrier semaphores. Data moves between devices by JAX's collectives and lax.ppermute only.
A program may use at most 64 MiB of HBM per device.

```python
import math
import jax
import jax.numpy as jnp
import numpy as np
from jax import lax

HEAD_TOTAL = 64
LATENT_WIDTH = 512
ROTARY_WIDTH = 64
QUERY_TOKENS = 1
REQUEST_SLOTS = 128
CACHE_POSITIONS = 768


def draw_cache(key, part):
    array_shape = (REQUEST_SLOTS, CACHE_POSITIONS, LATENT_WIDTH + ROTARY_WIDTH)
    value_rows = jnp.clip(jax.random.normal(jax.random.fold_in(key, 3), array_shape, jnp.float32), -4.0, 4.0)
    return value_rows.astype(jnp.bfloat16)


def draw_query(key, part):
    array_shape = (REQUEST_SLOTS, QUERY_TOKENS, HEAD_TOTAL, LATENT_WIDTH + ROTARY_WIDTH)
    value_rows = jnp.clip(0.6 * jax.random.normal(jax.random.fold_in(key, 5), array_shape, jnp.float32), -2.4, 2.4)
    return value_rows.astype(jnp.bfloat16)


def length_profile(count, total, bound, skew):
    loads = [(1 << 20) // math.isqrt(rank ** skew) + 1 for rank in range(2, count + 1)]
    rest, holding = total - bound - (count - 1), [1] * (count - 1)
    while rest > 0:
        free = [i for i in range(count - 1) if holding[i] < bound]
        whole, budget = sum([loads[i] for i in free]), rest
        for i in free:
            extra = min(bound - holding[i], max(1, budget * loads[i] // whole), rest)
            holding[i] = holding[i] + extra
            rest = rest - extra
    return np.array([bound] + holding)


def ragged_sizes(key, count, total, reach, slope):
    if count == 2:
        one = jax.random.randint(key, (), max(1, total - reach), min(reach, total - 1) + 1)
        return jnp.stack([one, total - one])
    sizes = jnp.asarray(length_profile(count, total, reach, slope), jnp.int32)
    couples = (count - 1) // 2
    donor, sink = sizes[1:1 + 2 * couples:2], sizes[2:2 + 2 * couples:2]
    margin = jnp.minimum(donor - 1, reach - sink)
    shifted = jax.random.randint(jax.random.fold_in(key, 1), (couples,), 0, 1 << 20) % (margin + 1)
    sizes = sizes.at[1:1 + 2 * couples:2].set(donor - shifted).at[2:2 + 2 * couples:2].set(sink + shifted)
    return sizes[jax.random.permutation(jax.random.fold_in(key, 2), count)]


def setup_inputs(seed: int = 0, part: int = 0) -> dict:
    seeds = jax.random.split(jax.random.key(seed), 5)
    part_keys = jax.random.split(jax.random.fold_in(seeds[4], part), 5)
    return {
        "cache": draw_cache(jax.random.fold_in(jax.random.fold_in(seeds[4], part), 71), part),
        "lengths": ragged_sizes(part_keys[1], REQUEST_SLOTS, REQUEST_SLOTS * CACHE_POSITIONS // 3, CACHE_POSITIONS - QUERY_TOKENS, 2).astype(jnp.int32),
        "slots": jax.random.permutation(part_keys[2], REQUEST_SLOTS).astype(jnp.int32),
        "query": draw_query(jax.random.fold_in(jax.random.fold_in(seeds[4], part), 71), part),
    }


def reference(cache, lengths, slots, query):
    score_scale = 0.0721687836
    owner = jnp.argsort(slots).astype(jnp.int32)
    positions = jnp.arange(CACHE_POSITIONS, dtype=jnp.int32)
    forward_steps = jnp.arange(QUERY_TOKENS, dtype=jnp.int32)

    def attend(slot_index):
        request = owner[slot_index]
        cache_key_rows = cache[request].astype(jnp.float32)
        query_rows = query[slot_index].astype(jnp.float32)
        scores = jnp.einsum("thc,pc->thp", query_rows, cache_key_rows) * score_scale
        key_limit = lengths[request] + forward_steps + 1
        visible = positions[None, None, :] < key_limit[:, None, None]
        scores = jnp.where(visible, scores, -1.0e30)
        highest = jnp.max(scores, axis=2, keepdims=True)
        softmax_weights = jnp.where(visible, jnp.exp(scores - highest), 0.0)
        weight_sum = jnp.sum(softmax_weights, axis=2)
        rounded_length = lax.optimization_barrier(softmax_weights.astype(jnp.bfloat16)).astype(jnp.float32)
        latent_total = jnp.einsum("seg,gr->ser", rounded_length, cache_key_rows[:, :LATENT_WIDTH])
        return (latent_total / weight_sum[..., None]).astype(jnp.bfloat16)

    return lax.map(attend, jnp.arange(REQUEST_SLOTS, dtype=jnp.int32))
```

```python
import jax
import jax.numpy as jnp
from jax import lax
from jax.experimental import pallas as pl
from jax.experimental.pallas import tpu as pltpu
from jax.sharding import PartitionSpec as P

LATENT_WIDTH = 512
COLUMNS = 4

score_scale = 0.0721687836
floor_value = -1e30

NT = (((1,), (1,)), ((), ()))
NN = (((1,), (0,)), ((), ()))


def pack_kernel(rows, slots_ref, cache_ref, packed_ref):
    count = slots_ref.shape[1]
    rotary = cache_ref.shape[1] - LATENT_WIDTH
    half, half_rotary = LATENT_WIDTH // 2, rotary // 2
    parts = []
    for h in range(2):
        parts.append(
            jnp.concatenate(
                [
                    cache_ref[h, :LATENT_WIDTH, :],
                    cache_ref[2, half * h : half * (h + 1), :],
                    cache_ref[h, LATENT_WIDTH:, :],
                    cache_ref[2, LATENT_WIDTH + half_rotary * h : LATENT_WIDTH + half_rotary * (h + 1), :],
                    jnp.zeros((half_rotary, count), cache_ref.dtype),
                ],
                axis=0,
            )
        )
    table = jnp.concatenate(parts, axis=1)
    slots = jnp.concatenate([slots_ref[...]] * 2, axis=1)
    row = lax.broadcasted_iota(jnp.int32, (2 * count, 1), 0)
    place = row // 2
    target = (place % COLUMNS) * rows + place // COLUMNS
    side = lax.broadcasted_iota(jnp.int32, (1, 2 * count), 1) // count
    chosen = (slots == target) & (side == row % 2)
    select = jnp.where(chosen, 1.0, 0.0).astype(cache_ref.dtype)
    packed_ref[...] = lax.dot_general(select, table, NT, preferred_element_type=jnp.float32).astype(
        packed_ref.dtype
    )


def attend_kernel(rows, me_ref, slots_ref, lengths_ref, query_ref, keys_ref, out_ref):
    heads = out_ref.shape[0]
    width = keys_ref.shape[0]
    half = LATENT_WIDTH // 2
    limit = 1 + jnp.sum(jnp.where(slots_ref[...] == me_ref[0], lengths_ref[...], 0), axis=1, keepdims=True)
    scores = lax.dot_general(query_ref[...], keys_ref[...], NT, preferred_element_type=jnp.float32) * score_scale
    lane = lax.broadcasted_iota(jnp.int32, (1, width), 1)
    side = lane % 2
    place = (lane // 2) % (width // 4)
    source = (place % COLUMNS) * rows + place // COLUMNS
    first = (source * 2 + lane // (width // 2)) * 3
    whole = scores[:heads]
    part = jnp.where(side == 0, scores[heads : 2 * heads], scores[2 * heads :])
    joined = part + jnp.where(side == 0, pltpu.roll(part, width - 1, 1), pltpu.roll(part, 1, 1))
    whole = jnp.where(first + side < limit, whole, floor_value)
    joined = jnp.where(first + 2 < limit, joined, floor_value)
    highest = jnp.max(jnp.maximum(whole, joined), axis=1, keepdims=True)
    whole = jnp.exp(whole - highest)
    joined = jnp.exp(joined - highest)
    even = jnp.where(side == 0, joined, 0.0)
    odd = joined - even
    weight_sum = jnp.sum(whole + even, axis=1, keepdims=True)
    latent = lax.dot_general(
        whole.astype(keys_ref.dtype), keys_ref[:, :LATENT_WIDTH], NN, preferred_element_type=jnp.float32
    )
    halves = lax.dot_general(
        jnp.concatenate([even, odd], axis=0).astype(keys_ref.dtype),
        keys_ref[:, LATENT_WIDTH : LATENT_WIDTH + half],
        NN,
        preferred_element_type=jnp.float32,
    )
    latent = latent + jnp.concatenate([halves[:heads], halves[heads:]], axis=1)
    out_ref[...] = (latent / weight_sum).astype(out_ref.dtype)


def shards(cache, lengths, slots, query):
    wide_count = lax.axis_size("wide")
    rows = wide_count // COLUMNS
    count = slots.shape[0]
    channels = cache.shape[2]
    rotary = channels - LATENT_WIDTH
    half, half_rotary = LATENT_WIDTH // 2, rotary // 2
    heads = query.shape[2]
    packed_width = LATENT_WIDTH + half + 2 * rotary
    slot_row = slots.reshape(1, count)
    length_row = lengths.reshape(1, count)
    packed = pl.pallas_call(
        lambda *refs: pack_kernel(rows, *refs),
        out_shape=jax.ShapeDtypeStruct((2 * count, packed_width), cache.dtype),
        name="pack",
    )(slot_row, jnp.transpose(cache, (1, 2, 0)))
    order = [x * rows + z for z in range(rows) for x in range(COLUMNS)]
    received = lax.all_to_all(
        packed.reshape(count, 2, packed_width), "wide", 0, 0, tiled=True, axis_index_groups=[order]
    )
    keys = lax.all_gather(received.reshape(2 * count, packed_width), "narrow", axis=0, tiled=True)
    q = query.reshape(heads, channels)
    latent, turned = q[:, :LATENT_WIDTH], q[:, LATENT_WIDTH:]

    def blank(n):
        return jnp.zeros((heads, n), q.dtype)

    stacked = [jnp.concatenate([latent, blank(half), turned, blank(rotary)], axis=1)]
    for h in range(2):
        stacked.append(
            jnp.concatenate(
                [
                    blank(LATENT_WIDTH),
                    latent[:, half * h : half * (h + 1)],
                    blank(rotary),
                    turned[:, half_rotary * h : half_rotary * (h + 1)],
                    blank(half_rotary),
                ],
                axis=1,
            )
        )
    queries = jnp.concatenate(stacked, axis=0)
    me = lax.axis_index("wide").astype(jnp.int32).reshape(1)
    vmem = pl.BlockSpec(memory_space=pltpu.VMEM)
    attended = pl.pallas_call(
        lambda *refs: attend_kernel(rows, *refs),
        out_shape=jax.ShapeDtypeStruct((heads, LATENT_WIDTH), jnp.bfloat16),
        in_specs=[pl.BlockSpec(memory_space=pltpu.SMEM), vmem, vmem, vmem, vmem],
        out_specs=vmem,
        name="attend",
    )(me, slot_row, length_row, queries, keys)
    return attended.reshape(1, 1, heads, LATENT_WIDTH)


def solution(mesh):
    return jax.shard_map(
        shards,
        mesh=mesh,
        in_specs=(
            P("grp", ("wide", "narrow"), None),
            P("grp"),
            P("grp"),
            P(("grp", "wide"), None, "narrow", None),
        ),
        out_specs=P(("grp", "wide"), None, "narrow", None),
        check_vma=False,
    )
```

```python
import jax
import jax.numpy as jnp
from jax import lax
from jax.experimental import pallas as pl
from jax.experimental.pallas import tpu as pltpu
from jax.sharding import PartitionSpec as P

LATENT_WIDTH = 512
COLUMNS = 4
VMEM_BYTES = 8 << 20

score_scale = 0.0721687836
floor_value = -1e30

NT = (((1,), (1,)), ((), ()))
NN = (((1,), (0,)), ((), ()))


def partner(place, rows):
    step, row = place // COLUMNS, 0
    for b in range(rows.bit_length() - 1):
        row = row * 2 + (step >> b) % 2
    return (place % COLUMNS) * rows + row


def pack_kernel(rows, slots_ref, cache_ref, packed_ref):
    count = slots_ref.shape[1]
    rotary = cache_ref.shape[1] - LATENT_WIDTH
    half, half_rotary = LATENT_WIDTH // 2, rotary // 2
    parts = []
    for h in range(2):
        parts.append(
            jnp.concatenate(
                [
                    cache_ref[h, :LATENT_WIDTH, :],
                    cache_ref[2, half * h : half * (h + 1), :],
                    cache_ref[h, LATENT_WIDTH:, :],
                    cache_ref[2, LATENT_WIDTH + half_rotary * h : LATENT_WIDTH + half_rotary * (h + 1), :],
                    jnp.zeros((half_rotary, count), cache_ref.dtype),
                ],
                axis=0,
            )
        )
    table = jnp.concatenate(parts, axis=1)
    slots = jnp.concatenate([slots_ref[...]] * 2, axis=1)
    row = lax.broadcasted_iota(jnp.int32, (2 * count, 1), 0)
    place = row // 2
    target = partner(place, rows)
    side = lax.broadcasted_iota(jnp.int32, (1, 2 * count), 1) // count
    chosen = (slots == target) & (side == row % 2)
    select = jnp.where(chosen, 1.0, 0.0).astype(cache_ref.dtype)
    packed = lax.dot_general(select, table, NT, preferred_element_type=jnp.float32).astype(packed_ref.dtype)
    packed_ref[...] = packed.reshape(packed_ref.shape)


def query_kernel(me_ref, slots_ref, lengths_ref, query_ref, stacked_ref, limit_ref):
    heads = query_ref.shape[0]
    rotary = query_ref.shape[1] - LATENT_WIDTH
    half, half_rotary = LATENT_WIDTH // 2, rotary // 2
    stacked_ref[...] = jnp.zeros_like(stacked_ref)
    tail = LATENT_WIDTH + half
    stacked_ref[:heads, :LATENT_WIDTH] = query_ref[:, :LATENT_WIDTH]
    stacked_ref[:heads, tail : tail + rotary] = query_ref[:, LATENT_WIDTH:]
    for h in range(2):
        rows = pl.ds(heads * (h + 1), heads)
        stacked_ref[rows, LATENT_WIDTH:tail] = query_ref[:, half * h : half * (h + 1)]
        stacked_ref[rows, tail + rotary : tail + rotary + half_rotary] = query_ref[
            :, LATENT_WIDTH + half_rotary * h : LATENT_WIDTH + half_rotary * (h + 1)
        ]
    own = jnp.where(slots_ref[...] == me_ref[0], lengths_ref[...], 0)
    limit_ref[...] = jnp.broadcast_to(1 + jnp.sum(own, axis=1, keepdims=True), limit_ref.shape)


def attend_kernel(rows, limit_ref, query_ref, keys_ref, out_ref):
    heads = out_ref.shape[0]
    width = keys_ref.shape[0]
    half = LATENT_WIDTH // 2
    limit = limit_ref[:, :1]
    scores = lax.dot_general(query_ref[...], keys_ref[...], NT, preferred_element_type=jnp.float32) * score_scale
    lane = lax.broadcasted_iota(jnp.int32, (1, width), 1)
    side = lane % 2
    place = (lane // 2) % (width // 4)
    source = partner(place, rows)
    first = (source * 2 + lane // (width // 2)) * 3
    whole = scores[:heads]
    part = jnp.where(side == 0, scores[heads : 2 * heads], scores[2 * heads :])
    joined = part + jnp.where(side == 0, pltpu.roll(part, width - 1, 1), pltpu.roll(part, 1, 1))
    whole = jnp.where(first + side < limit, whole, floor_value)
    joined = jnp.where(first + 2 < limit, joined, floor_value)
    highest = jnp.max(jnp.maximum(whole, joined), axis=1, keepdims=True)
    whole = jnp.exp(whole - highest)
    joined = jnp.exp(joined - highest)
    even = jnp.where(side == 0, joined, 0.0)
    odd = joined - even
    weight_sum = jnp.sum(whole + even, axis=1, keepdims=True)
    latent = lax.dot_general(
        whole.astype(keys_ref.dtype), keys_ref[:, :LATENT_WIDTH], NN, preferred_element_type=jnp.float32
    )
    halves = lax.dot_general(
        jnp.concatenate([even, odd], axis=0).astype(keys_ref.dtype),
        keys_ref[:, LATENT_WIDTH : LATENT_WIDTH + half],
        NN,
        preferred_element_type=jnp.float32,
    )
    latent = latent + jnp.concatenate([halves[:heads], halves[heads:]], axis=1)
    out_ref[...] = (latent / weight_sum).astype(out_ref.dtype)


def shards(cache, lengths, slots, query):
    wide_count = lax.axis_size("wide")
    rows = wide_count // COLUMNS
    count = slots.shape[0]
    channels = cache.shape[2]
    rotary = channels - LATENT_WIDTH
    heads = query.shape[2]
    packed_width = LATENT_WIDTH + LATENT_WIDTH // 2 + 2 * rotary
    slot_row = slots.reshape(1, count)
    packed = pl.pallas_call(
        lambda *refs: pack_kernel(rows, *refs),
        out_shape=jax.ShapeDtypeStruct((count, 2, packed_width), cache.dtype),
        name="pack",
    )(slot_row, jnp.transpose(cache, (1, 2, 0)))
    order = [partner(place, rows) for place in range(wide_count)]
    received = lax.all_to_all(
        packed, "wide", 0, 0, tiled=True, axis_index_groups=[order]
    )
    keys = lax.all_gather(received.reshape(2 * count, packed_width), "narrow", axis=0, tiled=True)
    me = lax.axis_index("wide").astype(jnp.int32).reshape(1)
    vmem = pl.BlockSpec(memory_space=pltpu.VMEM)
    stacked, limit = pl.pallas_call(
        query_kernel,
        out_shape=(
            jax.ShapeDtypeStruct((3 * heads, packed_width), query.dtype),
            jax.ShapeDtypeStruct((1, count), jnp.int32),
        ),
        in_specs=[pl.BlockSpec(memory_space=pltpu.SMEM), vmem, vmem, vmem],
        out_specs=(vmem, vmem),
        compiler_params=pltpu.CompilerParams(vmem_limit_bytes=VMEM_BYTES),
        cost_estimate=pl.CostEstimate(flops=1 << 22, bytes_accessed=1 << 18, transcendentals=0),
        name="stack",
    )(me, slot_row, lengths.reshape(1, count), query.reshape(heads, channels))
    attended = pl.pallas_call(
        lambda *refs: attend_kernel(rows, *refs),
        out_shape=jax.ShapeDtypeStruct((heads, LATENT_WIDTH), jnp.bfloat16),
        in_specs=[vmem, vmem, vmem],
        out_specs=vmem,
        compiler_params=pltpu.CompilerParams(vmem_limit_bytes=VMEM_BYTES),
        name="attend",
    )(limit, stacked, keys)
    return attended.reshape(1, 1, heads, LATENT_WIDTH)


def solution(mesh):
    return jax.shard_map(
        shards,
        mesh=mesh,
        in_specs=(
            P("grp", ("wide", "narrow"), None),
            P("grp"),
            P("grp"),
            P(("grp", "wide"), None, "narrow", None),
        ),
        out_specs=P(("grp", "wide"), None, "narrow", None),
        check_vma=False,
    )
```

```python
import jax
import jax.numpy as jnp
from jax import lax
from jax.experimental import pallas as pl
from jax.experimental.pallas import tpu as pltpu
from jax.sharding import PartitionSpec as P

LATENT_WIDTH = 512
COLUMNS = 4
VMEM_BYTES = 8 << 20

score_scale = 0.0721687836
floor_value = -1e30

NT = (((1,), (1,)), ((), ()))
NN = (((1,), (0,)), ((), ()))


def partner(place, rows):
    step, row = place // COLUMNS, 0
    for b in range(rows.bit_length() - 1):
        row = row * 2 + (step >> b) % 2
    return (place % COLUMNS) * rows + row


def pack_kernel(
    rows,
    slots_hbm,
    lengths_hbm,
    query_hbm,
    cache_hbm,
    packed_ref,
    stacked_ref,
    limit_ref,
    slots_ref,
    lengths_ref,
    query_ref,
    cache_ref,
    arrived,
):
    sources = (slots_hbm, cache_hbm, query_hbm, lengths_hbm)
    places = (slots_ref, cache_ref, query_ref, lengths_ref)
    copies = [pltpu.make_async_copy(a, b, arrived.at[i]) for i, (a, b) in enumerate(zip(sources, places))]
    for copy in copies:
        copy.start()
    count = slots_ref.shape[1]
    rotary = cache_ref.shape[1] - LATENT_WIDTH
    half, half_rotary = LATENT_WIDTH // 2, rotary // 2
    copies[0].wait()
    slots = jnp.concatenate([slots_ref[...]] * 2, axis=1)
    row = lax.broadcasted_iota(jnp.int32, (2 * count, 1), 0)
    place = row // 2
    target = partner(place, rows)
    side = lax.broadcasted_iota(jnp.int32, (1, 2 * count), 1) // count
    chosen = (slots == target) & (side == row % 2)
    select = jnp.where(chosen, 1.0, 0.0).astype(cache_ref.dtype)
    copies[1].wait()
    parts = []
    for h in range(2):
        parts.append(
            jnp.concatenate(
                [
                    cache_ref[h, :LATENT_WIDTH, :],
                    cache_ref[2, half * h : half * (h + 1), :],
                    cache_ref[h, LATENT_WIDTH:, :],
                    cache_ref[2, LATENT_WIDTH + half_rotary * h : LATENT_WIDTH + half_rotary * (h + 1), :],
                    jnp.zeros((half_rotary, count), cache_ref.dtype),
                ],
                axis=0,
            )
        )
    table = jnp.concatenate(parts, axis=1)
    packed = lax.dot_general(select, table, NT, preferred_element_type=jnp.float32).astype(packed_ref.dtype)
    packed_ref[...] = packed.reshape(packed_ref.shape)
    copies[2].wait()
    copies[3].wait()
    stack_queries(slots_ref, lengths_ref, query_ref, stacked_ref, limit_ref)


def stack_queries(slots_ref, lengths_ref, query_ref, stacked_ref, limit_ref):
    heads = query_ref.shape[0]
    rotary = query_ref.shape[1] - LATENT_WIDTH
    half, half_rotary = LATENT_WIDTH // 2, rotary // 2
    stacked_ref[...] = jnp.zeros_like(stacked_ref)
    tail = LATENT_WIDTH + half
    stacked_ref[:heads, :LATENT_WIDTH] = query_ref[:, :LATENT_WIDTH]
    stacked_ref[:heads, tail : tail + rotary] = query_ref[:, LATENT_WIDTH:]
    for h in range(2):
        rows = pl.ds(heads * (h + 1), heads)
        stacked_ref[rows, LATENT_WIDTH:tail] = query_ref[:, half * h : half * (h + 1)]
        stacked_ref[rows, tail + rotary : tail + rotary + half_rotary] = query_ref[
            :, LATENT_WIDTH + half_rotary * h : LATENT_WIDTH + half_rotary * (h + 1)
        ]
    own = jnp.where(slots_ref[...] == lax.axis_index("wide"), lengths_ref[...], 0)
    limit_ref[...] = jnp.broadcast_to(1 + jnp.sum(own, axis=1, keepdims=True), limit_ref.shape)


def attend_kernel(rows, limit_ref, query_ref, keys_ref, out_ref):
    heads = out_ref.shape[0]
    width = keys_ref.shape[0]
    half = LATENT_WIDTH // 2
    limit = limit_ref[:, :1]
    scores = lax.dot_general(query_ref[...], keys_ref[...], NT, preferred_element_type=jnp.float32) * score_scale
    lane = lax.broadcasted_iota(jnp.int32, (1, width), 1)
    side = lane % 2
    place = (lane // 2) % (width // 4)
    source = partner(place, rows)
    first = (source * 2 + lane // (width // 2)) * 3
    whole = scores[:heads]
    part = jnp.where(side == 0, scores[heads : 2 * heads], scores[2 * heads :])
    joined = part + jnp.where(side == 0, pltpu.roll(part, width - 1, 1), pltpu.roll(part, 1, 1))
    whole = jnp.where(first + side < limit, whole, floor_value)
    joined = jnp.where(first + 2 < limit, joined, floor_value)
    highest = jnp.max(jnp.maximum(whole, joined), axis=1, keepdims=True)
    whole = jnp.exp(whole - highest)
    joined = jnp.exp(joined - highest)
    even = jnp.where(side == 0, joined, 0.0)
    odd = joined - even
    weight_sum = jnp.sum(whole + even, axis=1, keepdims=True)
    latent = lax.dot_general(
        whole.astype(keys_ref.dtype), keys_ref[:, :LATENT_WIDTH], NN, preferred_element_type=jnp.float32
    )
    halves = lax.dot_general(
        jnp.concatenate([even, odd], axis=0).astype(keys_ref.dtype),
        keys_ref[:, LATENT_WIDTH : LATENT_WIDTH + half],
        NN,
        preferred_element_type=jnp.float32,
    )
    latent = latent + jnp.concatenate([halves[:heads], halves[heads:]], axis=1)
    out_ref[...] = (latent / weight_sum).astype(out_ref.dtype)


def shards(cache, lengths, slots, query):
    wide_count = lax.axis_size("wide")
    rows = wide_count // COLUMNS
    count = slots.shape[0]
    channels = cache.shape[2]
    rotary = channels - LATENT_WIDTH
    heads = query.shape[2]
    packed_width = LATENT_WIDTH + LATENT_WIDTH // 2 + 2 * rotary
    slot_row = slots.reshape(1, count)
    vmem = pl.BlockSpec(memory_space=pltpu.VMEM)
    hbm = pl.BlockSpec(memory_space=pltpu.HBM)

    def held(a):
        return pltpu.with_memory_space_constraint(a, pltpu.HBM)

    packed, stacked, limit = pl.pallas_call(
        lambda *refs: pack_kernel(rows, *refs),
        out_shape=(
            jax.ShapeDtypeStruct((count, 2, packed_width), cache.dtype),
            jax.ShapeDtypeStruct((3 * heads, packed_width), query.dtype),
            jax.ShapeDtypeStruct((1, count), jnp.int32),
        ),
        in_specs=[hbm, hbm, hbm, hbm],
        out_specs=(vmem, vmem, vmem),
        scratch_shapes=[
            pltpu.VMEM((1, count), jnp.int32),
            pltpu.VMEM((1, count), jnp.int32),
            pltpu.VMEM((heads, channels), query.dtype),
            pltpu.VMEM((cache.shape[1], channels, count), cache.dtype),
            pltpu.SemaphoreType.DMA((4,)),
        ],
        compiler_params=pltpu.CompilerParams(vmem_limit_bytes=VMEM_BYTES),
        name="pack",
    )(
        held(slot_row),
        held(lengths.reshape(1, count)),
        held(query.reshape(heads, channels)),
        held(jnp.transpose(cache, (1, 2, 0))),
    )
    order = [partner(place, rows) for place in range(wide_count)]
    received = lax.all_to_all(
        packed, "wide", 0, 0, tiled=True, axis_index_groups=[order]
    )
    keys = lax.all_gather(received.reshape(2 * count, packed_width), "narrow", axis=0, tiled=True)
    attended = pl.pallas_call(
        lambda *refs: attend_kernel(rows, *refs),
        out_shape=jax.ShapeDtypeStruct((heads, LATENT_WIDTH), jnp.bfloat16),
        in_specs=[vmem, vmem, vmem],
        out_specs=vmem,
        compiler_params=pltpu.CompilerParams(vmem_limit_bytes=VMEM_BYTES),
        name="attend",
    )(limit, stacked, keys)
    return attended.reshape(1, 1, heads, LATENT_WIDTH)


def solution(mesh):
    return jax.shard_map(
        shards,
        mesh=mesh,
        in_specs=(
            P("grp", ("wide", "narrow"), None),
            P("grp"),
            P("grp"),
            P(("grp", "wide"), None, "narrow", None),
        ),
        out_specs=P(("grp", "wide"), None, "narrow", None),
        check_vma=False,
    )
```

```python
import jax
import jax.numpy as jnp
from jax import lax
from jax.experimental import pallas as pl
from jax.experimental.pallas import tpu as pltpu
from jax.sharding import PartitionSpec as P

LATENT_WIDTH = 512
COLUMNS = 4
VMEM_BYTES = 8 << 20

score_scale = 0.0721687836
floor_value = -1e30

NT = (((1,), (1,)), ((), ()))
NN = (((1,), (0,)), ((), ()))


def partner(place, rows):
    step = place // COLUMNS
    run = step % 4
    row = step // 4 + (run % 2) * (rows // 2) + (run // 2) * (rows // 4)
    return (place % COLUMNS) * rows + row


def pack_kernel(
    rows,
    slots_hbm,
    lengths_hbm,
    query_hbm,
    cache_hbm,
    packed_ref,
    stacked_ref,
    limit_ref,
    slots_ref,
    lengths_ref,
    query_ref,
    cache_ref,
    arrived,
):
    sources = (slots_hbm, cache_hbm, query_hbm, lengths_hbm)
    places = (slots_ref, cache_ref, query_ref, lengths_ref)
    copies = [pltpu.make_async_copy(a, b, arrived.at[i]) for i, (a, b) in enumerate(zip(sources, places))]
    for copy in copies:
        copy.start()
    count = slots_ref.shape[1]
    rotary = cache_ref.shape[1] - LATENT_WIDTH
    half, half_rotary = LATENT_WIDTH // 2, rotary // 2
    copies[0].wait()
    slots = jnp.concatenate([slots_ref[...]] * 2, axis=1)
    row = lax.broadcasted_iota(jnp.int32, (2 * count, 1), 0)
    place = row // 2
    target = partner(place, rows)
    side = lax.broadcasted_iota(jnp.int32, (1, 2 * count), 1) // count
    chosen = (slots == target) & (side == row % 2)
    select = jnp.where(chosen, 1.0, 0.0).astype(cache_ref.dtype)
    copies[1].wait()
    parts = []
    for h in range(2):
        parts.append(
            jnp.concatenate(
                [
                    cache_ref[h, :LATENT_WIDTH, :],
                    cache_ref[2, half * h : half * (h + 1), :],
                    cache_ref[h, LATENT_WIDTH:, :],
                    cache_ref[2, LATENT_WIDTH + half_rotary * h : LATENT_WIDTH + half_rotary * (h + 1), :],
                    jnp.zeros((half_rotary, count), cache_ref.dtype),
                ],
                axis=0,
            )
        )
    table = jnp.concatenate(parts, axis=1)
    packed = lax.dot_general(select, table, NT, preferred_element_type=jnp.float32).astype(packed_ref.dtype)
    packed_ref[...] = packed.reshape(packed_ref.shape)
    copies[2].wait()
    copies[3].wait()
    stack_queries(slots_ref, lengths_ref, query_ref, stacked_ref, limit_ref)


def stack_queries(slots_ref, lengths_ref, query_ref, stacked_ref, limit_ref):
    heads = query_ref.shape[0]
    rotary = query_ref.shape[1] - LATENT_WIDTH
    half, half_rotary = LATENT_WIDTH // 2, rotary // 2
    stacked_ref[...] = jnp.zeros_like(stacked_ref)
    tail = LATENT_WIDTH + half
    stacked_ref[:heads, :LATENT_WIDTH] = query_ref[:, :LATENT_WIDTH]
    stacked_ref[:heads, tail : tail + rotary] = query_ref[:, LATENT_WIDTH:]
    for h in range(2):
        rows = pl.ds(heads * (h + 1), heads)
        stacked_ref[rows, LATENT_WIDTH:tail] = query_ref[:, half * h : half * (h + 1)]
        stacked_ref[rows, tail + rotary : tail + rotary + half_rotary] = query_ref[
            :, LATENT_WIDTH + half_rotary * h : LATENT_WIDTH + half_rotary * (h + 1)
        ]
    own = jnp.where(slots_ref[...] == lax.axis_index("wide"), lengths_ref[...], 0)
    limit_ref[...] = jnp.broadcast_to(1 + jnp.sum(own, axis=1, keepdims=True), limit_ref.shape)


def attend_kernel(rows, limit_ref, query_ref, keys_ref, out_ref):
    heads = out_ref.shape[0]
    keys = keys_ref[...].reshape(2 * keys_ref.shape[0], keys_ref.shape[2])
    width = keys.shape[0]
    half = LATENT_WIDTH // 2
    limit = limit_ref[:, :1]
    scores = lax.dot_general(query_ref[...], keys, NT, preferred_element_type=jnp.float32) * score_scale
    lane = lax.broadcasted_iota(jnp.int32, (1, width), 1)
    side = lane % 2
    place = (lane // 2) % (width // 4)
    source = partner(place, rows)
    first = (source * 2 + lane // (width // 2)) * 3
    whole = scores[:heads]
    part = jnp.where(side == 0, scores[heads : 2 * heads], scores[2 * heads :])
    joined = part + jnp.where(side == 0, pltpu.roll(part, width - 1, 1), pltpu.roll(part, 1, 1))
    whole = jnp.where(first + side < limit, whole, floor_value)
    joined = jnp.where(first + 2 < limit, joined, floor_value)
    highest = jnp.max(jnp.maximum(whole, joined), axis=1, keepdims=True)
    whole = jnp.exp(whole - highest)
    joined = jnp.exp(joined - highest)
    even = jnp.where(side == 0, joined, 0.0)
    odd = joined - even
    weight_sum = jnp.sum(whole + even, axis=1, keepdims=True)
    latent = lax.dot_general(
        whole.astype(keys.dtype), keys[:, :LATENT_WIDTH], NN, preferred_element_type=jnp.float32
    )
    halves = lax.dot_general(
        jnp.concatenate([even, odd], axis=0).astype(keys.dtype),
        keys[:, LATENT_WIDTH : LATENT_WIDTH + half],
        NN,
        preferred_element_type=jnp.float32,
    )
    latent = latent + jnp.concatenate([halves[:heads], halves[heads:]], axis=1)
    out_ref[...] = (latent / weight_sum).astype(out_ref.dtype)


def shards(cache, lengths, slots, query):
    wide_count = lax.axis_size("wide")
    rows = wide_count // COLUMNS
    count = slots.shape[0]
    channels = cache.shape[2]
    rotary = channels - LATENT_WIDTH
    heads = query.shape[2]
    packed_width = LATENT_WIDTH + LATENT_WIDTH // 2 + 2 * rotary
    slot_row = slots.reshape(1, count)
    vmem = pl.BlockSpec(memory_space=pltpu.VMEM)
    hbm = pl.BlockSpec(memory_space=pltpu.HBM)

    def held(a):
        return pltpu.with_memory_space_constraint(a, pltpu.HBM)

    packed, stacked, limit = pl.pallas_call(
        lambda *refs: pack_kernel(rows, *refs),
        out_shape=(
            jax.ShapeDtypeStruct((count, 2, packed_width), cache.dtype),
            jax.ShapeDtypeStruct((3 * heads, packed_width), query.dtype),
            jax.ShapeDtypeStruct((1, count), jnp.int32),
        ),
        in_specs=[hbm, hbm, hbm, hbm],
        out_specs=(vmem, vmem, vmem),
        scratch_shapes=[
            pltpu.VMEM((1, count), jnp.int32),
            pltpu.VMEM((1, count), jnp.int32),
            pltpu.VMEM((heads, channels), query.dtype),
            pltpu.VMEM((cache.shape[1], channels, count), cache.dtype),
            pltpu.SemaphoreType.DMA((4,)),
        ],
        compiler_params=pltpu.CompilerParams(vmem_limit_bytes=VMEM_BYTES),
        name="pack",
    )(
        held(slot_row),
        held(lengths.reshape(1, count)),
        held(query.reshape(heads, channels)),
        held(jnp.transpose(cache, (1, 2, 0))),
    )
    order = [partner(place, rows) for place in range(wide_count)]
    received = lax.all_to_all(
        packed, "wide", 0, 0, tiled=True, axis_index_groups=[order]
    )
    keys = lax.all_gather(received, "narrow", axis=0, tiled=True)
    attended = pl.pallas_call(
        lambda *refs: attend_kernel(rows, *refs),
        out_shape=jax.ShapeDtypeStruct((heads, LATENT_WIDTH), jnp.bfloat16),
        in_specs=[vmem, vmem, vmem],
        out_specs=vmem,
        compiler_params=pltpu.CompilerParams(vmem_limit_bytes=VMEM_BYTES),
        name="attend",
    )(limit, stacked, keys)
    return attended.reshape(1, 1, heads, LATENT_WIDTH)


def solution(mesh):
    return jax.shard_map(
        shards,
        mesh=mesh,
        in_specs=(
            P("grp", ("wide", "narrow"), None),
            P("grp"),
            P("grp"),
            P(("grp", "wide"), None, "narrow", None),
        ),
        out_specs=P(("grp", "wide"), None, "narrow", None),
        check_vma=False,
    )
```

```python
import jax
import jax.numpy as jnp
from jax import lax
from jax.experimental import pallas as pl
from jax.experimental.pallas import tpu as pltpu
from jax.sharding import PartitionSpec as P

LATENT_WIDTH = 512
COLUMNS = 4
VMEM_BYTES = 8 << 20

score_scale = 0.0721687836
floor_value = -1e30

NT = (((1,), (1,)), ((), ()))
NN = (((1,), (0,)), ((), ()))


def partner(place, rows):
    step = place // COLUMNS
    run, turn = step % 4, step // 4
    row = turn + (run % 2) * (rows // 2) + (run // 2) * (rows // 4)
    row = row + (run // 3) * (rows // 4 - 1 - 2 * turn)
    return (place % COLUMNS) * rows + row


def pack_kernel(
    rows,
    slots_hbm,
    lengths_hbm,
    query_hbm,
    cache_hbm,
    packed_ref,
    stacked_ref,
    limit_ref,
    slots_ref,
    lengths_ref,
    query_ref,
    cache_ref,
    arrived,
):
    sources = (slots_hbm, query_hbm, lengths_hbm, cache_hbm)
    places = (slots_ref, query_ref, lengths_ref, cache_ref)
    copies = [pltpu.make_async_copy(a, b, arrived.at[i]) for i, (a, b) in enumerate(zip(sources, places))]
    for copy in copies:
        copy.start()
    count = slots_ref.shape[1]
    rotary = cache_ref.shape[1] - LATENT_WIDTH
    half, half_rotary = LATENT_WIDTH // 2, rotary // 2
    copies[0].wait()
    slots = jnp.concatenate([slots_ref[...]] * 2, axis=1)
    row = lax.broadcasted_iota(jnp.int32, (2 * count, 1), 0)
    place = row // 2
    target = partner(place, rows)
    side = lax.broadcasted_iota(jnp.int32, (1, 2 * count), 1) // count
    chosen = (slots == target) & (side == row % 2)
    select = jnp.where(chosen, 1.0, 0.0).astype(cache_ref.dtype)
    copies[1].wait()
    copies[2].wait()
    stack_queries(slots_ref, lengths_ref, query_ref, stacked_ref, limit_ref)
    copies[3].wait()
    parts = []
    for h in range(2):
        parts.append(
            jnp.concatenate(
                [
                    cache_ref[h, :LATENT_WIDTH, :],
                    cache_ref[2, half * h : half * (h + 1), :],
                    cache_ref[h, LATENT_WIDTH:, :],
                    cache_ref[2, LATENT_WIDTH + half_rotary * h : LATENT_WIDTH + half_rotary * (h + 1), :],
                    jnp.zeros((half_rotary, count), cache_ref.dtype),
                ],
                axis=0,
            )
        )
    table = jnp.concatenate(parts, axis=1)
    packed = lax.dot_general(select, table, NT, preferred_element_type=jnp.float32).astype(packed_ref.dtype)
    packed_ref[...] = packed.reshape(packed_ref.shape)


def stack_queries(slots_ref, lengths_ref, query_ref, stacked_ref, limit_ref):
    heads = query_ref.shape[0]
    rotary = query_ref.shape[1] - LATENT_WIDTH
    half, half_rotary = LATENT_WIDTH // 2, rotary // 2
    stacked_ref[...] = jnp.zeros_like(stacked_ref)
    tail = LATENT_WIDTH + half
    stacked_ref[:heads, :LATENT_WIDTH] = query_ref[:, :LATENT_WIDTH]
    stacked_ref[:heads, tail : tail + rotary] = query_ref[:, LATENT_WIDTH:]
    for h in range(2):
        rows = pl.ds(heads * (h + 1), heads)
        stacked_ref[rows, LATENT_WIDTH:tail] = query_ref[:, half * h : half * (h + 1)]
        stacked_ref[rows, tail + rotary : tail + rotary + half_rotary] = query_ref[
            :, LATENT_WIDTH + half_rotary * h : LATENT_WIDTH + half_rotary * (h + 1)
        ]
    own = jnp.where(slots_ref[...] == lax.axis_index("wide"), lengths_ref[...], 0)
    limit_ref[...] = jnp.broadcast_to(1 + jnp.sum(own, axis=1, keepdims=True), limit_ref.shape)


def attend_kernel(rows, limit_ref, query_ref, keys_ref, out_ref):
    heads = out_ref.shape[0]
    keys = keys_ref[...].reshape(2 * keys_ref.shape[0], keys_ref.shape[2])
    width = keys.shape[0]
    half = LATENT_WIDTH // 2
    limit = limit_ref[:, :1]
    scores = lax.dot_general(query_ref[...], keys, NT, preferred_element_type=jnp.float32) * score_scale
    lane = lax.broadcasted_iota(jnp.int32, (1, width), 1)
    side = lane % 2
    place = (lane // 2) % (width // 4)
    source = partner(place, rows)
    first = (source * 2 + lane // (width // 2)) * 3
    whole = scores[:heads]
    part = jnp.where(side == 0, scores[heads : 2 * heads], scores[2 * heads :])
    joined = part + jnp.where(side == 0, pltpu.roll(part, width - 1, 1), pltpu.roll(part, 1, 1))
    whole = jnp.where(first + side < limit, whole, floor_value)
    joined = jnp.where(first + 2 < limit, joined, floor_value)
    highest = jnp.max(jnp.maximum(whole, joined), axis=1, keepdims=True)
    whole = jnp.exp(whole - highest)
    joined = jnp.exp(joined - highest)
    even = jnp.where(side == 0, joined, 0.0)
    odd = joined - even
    weight_sum = jnp.sum(whole + even, axis=1, keepdims=True)
    latent = lax.dot_general(
        whole.astype(keys.dtype), keys[:, :LATENT_WIDTH], NN, preferred_element_type=jnp.float32
    )
    halves = lax.dot_general(
        jnp.concatenate([even, odd], axis=0).astype(keys.dtype),
        keys[:, LATENT_WIDTH : LATENT_WIDTH + half],
        NN,
        preferred_element_type=jnp.float32,
    )
    latent = latent + jnp.concatenate([halves[:heads], halves[heads:]], axis=1)
    out_ref[...] = (latent / weight_sum).astype(out_ref.dtype)


def shards(cache, lengths, slots, query):
    wide_count = lax.axis_size("wide")
    rows = wide_count // COLUMNS
    count = slots.shape[0]
    channels = cache.shape[2]
    rotary = channels - LATENT_WIDTH
    heads = query.shape[2]
    packed_width = LATENT_WIDTH + LATENT_WIDTH // 2 + 2 * rotary
    slot_row = slots.reshape(1, count)
    vmem = pl.BlockSpec(memory_space=pltpu.VMEM)
    hbm = pl.BlockSpec(memory_space=pltpu.HBM)

    def held(a):
        return pltpu.with_memory_space_constraint(a, pltpu.HBM)

    packed, stacked, limit = pl.pallas_call(
        lambda *refs: pack_kernel(rows, *refs),
        out_shape=(
            jax.ShapeDtypeStruct((count, 2, packed_width), cache.dtype),
            jax.ShapeDtypeStruct((3 * heads, packed_width), query.dtype),
            jax.ShapeDtypeStruct((1, count), jnp.int32),
        ),
        in_specs=[hbm, hbm, hbm, hbm],
        out_specs=(vmem, vmem, vmem),
        scratch_shapes=[
            pltpu.VMEM((1, count), jnp.int32),
            pltpu.VMEM((1, count), jnp.int32),
            pltpu.VMEM((heads, channels), query.dtype),
            pltpu.VMEM((cache.shape[1], channels, count), cache.dtype),
            pltpu.SemaphoreType.DMA((4,)),
        ],
        compiler_params=pltpu.CompilerParams(vmem_limit_bytes=VMEM_BYTES),
        name="pack",
    )(
        held(slot_row),
        held(lengths.reshape(1, count)),
        held(query.reshape(heads, channels)),
        held(jnp.transpose(cache, (1, 2, 0))),
    )
    order = [partner(place, rows) for place in range(wide_count)]
    received = lax.all_to_all(
        packed, "wide", 0, 0, tiled=True, axis_index_groups=[order]
    )
    keys = lax.all_gather(received, "narrow", axis=0, tiled=True)
    attended = pl.pallas_call(
        lambda *refs: attend_kernel(rows, *refs),
        out_shape=jax.ShapeDtypeStruct((heads, LATENT_WIDTH), jnp.bfloat16),
        in_specs=[vmem, vmem, vmem],
        out_specs=vmem,
        compiler_params=pltpu.CompilerParams(vmem_limit_bytes=VMEM_BYTES),
        name="attend",
    )(limit, stacked, keys)
    return attended.reshape(1, 1, heads, LATENT_WIDTH)


def solution(mesh):
    return jax.shard_map(
        shards,
        mesh=mesh,
        in_specs=(
            P("grp", ("wide", "narrow"), None),
            P("grp"),
            P("grp"),
            P(("grp", "wide"), None, "narrow", None),
        ),
        out_specs=P(("grp", "wide"), None, "narrow", None),
        check_vma=False,
    )
```

```python
import jax
import jax.numpy as jnp
from jax import lax
from jax.experimental import pallas as pl
from jax.experimental.pallas import tpu as pltpu
from jax.sharding import PartitionSpec as P

LATENT_WIDTH = 512
COLUMNS = 4
VMEM_BYTES = 8 << 20

score_scale = 0.0721687836
floor_value = -1e30

NT = (((1,), (1,)), ((), ()))
NN = (((1,), (0,)), ((), ()))


def partner(place, rows):
    step = place // COLUMNS
    run, turn = step % 4, step // 4
    row = turn + (run % 2) * (rows // 2) + (run // 2) * (rows // 4)
    row = row + (run // 3) * (rows // 4 - 1 - 2 * turn)
    return (place % COLUMNS) * rows + row


def place_of(wide, rows):
    column, row = wide // rows, wide % rows
    quarter, turn = row // (rows // 4), row % (rows // 4)
    run = quarter % 2 * 2 + quarter // 2
    turn = turn + (quarter // 3) * (rows // 4 - 1 - 2 * turn)
    return (turn * 4 + run) * COLUMNS + column


def pack_kernel(
    rows,
    slots_hbm,
    lengths_hbm,
    query_hbm,
    cache_hbm,
    packed_ref,
    stacked_ref,
    limit_ref,
    slots_ref,
    lengths_ref,
    query_ref,
    cache_ref,
    arrived,
):
    sources = (slots_hbm, query_hbm, lengths_hbm, cache_hbm)
    places = (slots_ref, query_ref, lengths_ref, cache_ref)
    copies = [pltpu.make_async_copy(a, b, arrived.at[i]) for i, (a, b) in enumerate(zip(sources, places))]
    for copy in copies:
        copy.start()
    count = slots_ref.shape[1]
    rotary = cache_ref.shape[1] - LATENT_WIDTH
    half, half_rotary = LATENT_WIDTH // 2, rotary // 2
    copies[0].wait()
    places_of = place_of(slots_ref[...], rows)
    lane_key = jnp.concatenate([2 * places_of, 2 * places_of + 1], axis=1)
    chosen = lane_key == lax.broadcasted_iota(jnp.int32, (2 * count, 2 * count), 0)
    select = jnp.where(chosen, 1.0, 0.0).astype(cache_ref.dtype)
    copies[1].wait()
    copies[2].wait()
    stack_queries(slots_ref, lengths_ref, query_ref, stacked_ref, limit_ref)
    copies[3].wait()
    parts = []
    for h in range(2):
        parts.append(
            jnp.concatenate(
                [
                    cache_ref[h, :LATENT_WIDTH, :],
                    cache_ref[2, half * h : half * (h + 1), :],
                    cache_ref[h, LATENT_WIDTH:, :],
                    cache_ref[2, LATENT_WIDTH + half_rotary * h : LATENT_WIDTH + half_rotary * (h + 1), :],
                    jnp.zeros((half_rotary, count), cache_ref.dtype),
                ],
                axis=0,
            )
        )
    table = jnp.concatenate(parts, axis=1)
    packed = lax.dot_general(select, table, NT, preferred_element_type=jnp.float32).astype(packed_ref.dtype)
    packed_ref[...] = packed.reshape(packed_ref.shape)


def stack_queries(slots_ref, lengths_ref, query_ref, stacked_ref, limit_ref):
    heads = query_ref.shape[0]
    rotary = query_ref.shape[1] - LATENT_WIDTH
    half, half_rotary = LATENT_WIDTH // 2, rotary // 2
    latent = query_ref[:, :LATENT_WIDTH]
    turned = query_ref[:, LATENT_WIDTH:].astype(jnp.float32)
    turned = jnp.concatenate([turned, jnp.zeros_like(turned)], axis=1)
    lane = lax.broadcasted_iota(jnp.int32, (1, 2 * rotary), 1)
    shared = (lane >= rotary) & (lane < rotary + half_rotary)

    def blank(n):
        return jnp.zeros((heads, n), latent.dtype)

    stacked_ref[:heads] = jnp.concatenate([latent, blank(half), turned.astype(latent.dtype)], axis=1)
    for h in range(2):
        moved = jnp.where(shared, pltpu.roll(turned, rotary - half_rotary * h, 1), 0.0)
        part = latent[:, half * h : half * (h + 1)]
        stacked_ref[heads * (h + 1) : heads * (h + 2)] = jnp.concatenate(
            [blank(LATENT_WIDTH), part, moved.astype(latent.dtype)], axis=1
        )
    own = jnp.where(slots_ref[...] == lax.axis_index("wide"), lengths_ref[...], 0)
    limit_ref[...] = jnp.broadcast_to(1 + jnp.sum(own, axis=1, keepdims=True), limit_ref.shape)


def attend_kernel(rows, limit_ref, query_ref, keys_ref, out_ref):
    heads = out_ref.shape[0]
    keys = keys_ref[...].reshape(2 * keys_ref.shape[0], keys_ref.shape[2])
    width = keys.shape[0]
    half = LATENT_WIDTH // 2
    limit = limit_ref[:, :1]
    scores = lax.dot_general(query_ref[...], keys, NT, preferred_element_type=jnp.float32) * score_scale
    lane = lax.broadcasted_iota(jnp.int32, (1, width), 1)
    side = lane % 2
    place = (lane // 2) % (width // 4)
    source = partner(place, rows)
    first = (source * 2 + lane // (width // 2)) * 3
    whole = scores[:heads]
    part = jnp.where(side == 0, scores[heads : 2 * heads], scores[2 * heads :])
    joined = part + jnp.where(side == 0, pltpu.roll(part, width - 1, 1), pltpu.roll(part, 1, 1))
    whole = jnp.where(first + side < limit, whole, floor_value)
    joined = jnp.where(first + 2 < limit, joined, floor_value)
    highest = jnp.max(jnp.maximum(whole, joined), axis=1, keepdims=True)
    whole = jnp.exp(whole - highest)
    joined = jnp.exp(joined - highest)
    even = jnp.where(side == 0, joined, 0.0)
    odd = joined - even
    weight_sum = jnp.sum(whole + even, axis=1, keepdims=True)
    latent = lax.dot_general(
        whole.astype(keys.dtype), keys[:, :LATENT_WIDTH], NN, preferred_element_type=jnp.float32
    )
    halves = lax.dot_general(
        jnp.concatenate([even, odd], axis=0).astype(keys.dtype),
        keys[:, LATENT_WIDTH : LATENT_WIDTH + half],
        NN,
        preferred_element_type=jnp.float32,
    )
    latent = latent + jnp.concatenate([halves[:heads], halves[heads:]], axis=1)
    out_ref[...] = (latent / weight_sum).astype(out_ref.dtype)


def shards(cache, lengths, slots, query):
    wide_count = lax.axis_size("wide")
    rows = wide_count // COLUMNS
    count = slots.shape[0]
    channels = cache.shape[2]
    rotary = channels - LATENT_WIDTH
    heads = query.shape[2]
    packed_width = LATENT_WIDTH + LATENT_WIDTH // 2 + 2 * rotary
    slot_row = slots.reshape(1, count)
    vmem = pl.BlockSpec(memory_space=pltpu.VMEM)
    hbm = pl.BlockSpec(memory_space=pltpu.HBM)

    def held(a):
        return pltpu.with_memory_space_constraint(a, pltpu.HBM)

    packed, stacked, limit = pl.pallas_call(
        lambda *refs: pack_kernel(rows, *refs),
        out_shape=(
            jax.ShapeDtypeStruct((count, 2, packed_width), cache.dtype),
            jax.ShapeDtypeStruct((3 * heads, packed_width), query.dtype),
            jax.ShapeDtypeStruct((1, count), jnp.int32),
        ),
        in_specs=[hbm, hbm, hbm, hbm],
        out_specs=(vmem, vmem, vmem),
        scratch_shapes=[
            pltpu.VMEM((1, count), jnp.int32),
            pltpu.VMEM((1, count), jnp.int32),
            pltpu.VMEM((heads, channels), query.dtype),
            pltpu.VMEM((cache.shape[1], channels, count), cache.dtype),
            pltpu.SemaphoreType.DMA((4,)),
        ],
        compiler_params=pltpu.CompilerParams(vmem_limit_bytes=VMEM_BYTES),
        name="pack",
    )(
        held(slot_row),
        held(lengths.reshape(1, count)),
        held(query.reshape(heads, channels)),
        held(jnp.transpose(cache, (1, 2, 0))),
    )
    order = [partner(place, rows) for place in range(wide_count)]
    received = lax.all_to_all(
        packed, "wide", 0, 0, tiled=True, axis_index_groups=[order]
    )
    keys = lax.all_gather(received, "narrow", axis=0, tiled=True)
    attended = pl.pallas_call(
        lambda *refs: attend_kernel(rows, *refs),
        out_shape=jax.ShapeDtypeStruct((heads, LATENT_WIDTH), jnp.bfloat16),
        in_specs=[vmem, vmem, vmem],
        out_specs=vmem,
        compiler_params=pltpu.CompilerParams(vmem_limit_bytes=VMEM_BYTES),
        name="attend",
    )(limit, stacked, keys)
    return attended.reshape(1, 1, heads, LATENT_WIDTH)


def solution(mesh):
    return jax.shard_map(
        shards,
        mesh=mesh,
        in_specs=(
            P("grp", ("wide", "narrow"), None),
            P("grp"),
            P("grp"),
            P(("grp", "wide"), None, "narrow", None),
        ),
        out_specs=P(("grp", "wide"), None, "narrow", None),
        check_vma=False,
    )
```

```python
import jax
import jax.numpy as jnp
from jax import lax
from jax.experimental import pallas as pl
from jax.experimental.pallas import tpu as pltpu
from jax.sharding import PartitionSpec as P

LATENT_WIDTH = 512
COLUMNS = 4
VMEM_BYTES = 8 << 20

score_scale = 0.0721687836
floor_value = -1e30

NT = (((1,), (1,)), ((), ()))
NN = (((1,), (0,)), ((), ()))


def partner(place, rows):
    step = place // COLUMNS
    run, turn = step % 4, step // 4
    row = turn + (run % 2) * (rows // 2) + (run // 2) * (rows // 4)
    row = row + (run // 3) * (rows // 4 - 1 - 2 * turn)
    return (place % COLUMNS) * rows + row


def place_of(wide, rows):
    column, row = wide // rows, wide % rows
    quarter, turn = row // (rows // 4), row % (rows // 4)
    run = quarter % 2 * 2 + quarter // 2
    turn = turn + (quarter // 3) * (rows // 4 - 1 - 2 * turn)
    return (turn * 4 + run) * COLUMNS + column


def pack_kernel(
    rows,
    slots_hbm,
    lengths_hbm,
    query_hbm,
    cache_hbm,
    packed_ref,
    stacked_ref,
    visible_ref,
    slots_ref,
    lengths_ref,
    query_ref,
    cache_ref,
    arrived,
):
    sources = (slots_hbm, query_hbm, lengths_hbm, cache_hbm)
    places = (slots_ref, query_ref, lengths_ref, cache_ref)
    copies = [pltpu.make_async_copy(a, b, arrived.at[i]) for i, (a, b) in enumerate(zip(sources, places))]
    for copy in copies:
        copy.start()
    count = slots_ref.shape[1]
    rotary = cache_ref.shape[1] - LATENT_WIDTH
    half, half_rotary = LATENT_WIDTH // 2, rotary // 2
    copies[0].wait()
    places_of = place_of(slots_ref[...], rows)
    lane_key = jnp.concatenate([2 * places_of, 2 * places_of + 1], axis=1)
    chosen = lane_key == lax.broadcasted_iota(jnp.int32, (2 * count, 2 * count), 0)
    select = jnp.where(chosen, 1.0, 0.0).astype(cache_ref.dtype)
    copies[1].wait()
    copies[2].wait()
    stack_queries(rows, slots_ref, lengths_ref, query_ref, stacked_ref, visible_ref)
    copies[3].wait()
    parts = []
    for h in range(2):
        parts.append(
            jnp.concatenate(
                [
                    cache_ref[h, :LATENT_WIDTH, :],
                    cache_ref[2, half * h : half * (h + 1), :],
                    cache_ref[h, LATENT_WIDTH:, :],
                    cache_ref[2, LATENT_WIDTH + half_rotary * h : LATENT_WIDTH + half_rotary * (h + 1), :],
                    jnp.zeros((half_rotary, count), cache_ref.dtype),
                ],
                axis=0,
            )
        )
    table = jnp.concatenate(parts, axis=1)
    packed = lax.dot_general(select, table, NT, preferred_element_type=jnp.float32).astype(packed_ref.dtype)
    packed_ref[...] = packed.reshape(packed_ref.shape)


def stack_queries(wide_rows, slots_ref, lengths_ref, query_ref, stacked_ref, visible_ref):
    heads = query_ref.shape[0]
    rotary = query_ref.shape[1] - LATENT_WIDTH
    half, half_rotary = LATENT_WIDTH // 2, rotary // 2
    latent = query_ref[:, :LATENT_WIDTH]
    turned = query_ref[:, LATENT_WIDTH:].astype(jnp.float32)
    turned = jnp.concatenate([turned, jnp.zeros_like(turned)], axis=1)
    lane = lax.broadcasted_iota(jnp.int32, (1, 2 * rotary), 1)
    shared = (lane >= rotary) & (lane < rotary + half_rotary)

    def blank(n):
        return jnp.zeros((heads, n), latent.dtype)

    stacked_ref[:heads] = jnp.concatenate([latent, blank(half), turned.astype(latent.dtype)], axis=1)
    for h in range(2):
        moved = jnp.where(shared, pltpu.roll(turned, rotary - half_rotary * h, 1), 0.0)
        part = latent[:, half * h : half * (h + 1)]
        stacked_ref[heads * (h + 1) : heads * (h + 2)] = jnp.concatenate(
            [blank(LATENT_WIDTH), part, moved.astype(latent.dtype)], axis=1
        )
    own = jnp.where(slots_ref[...] == lax.axis_index("wide"), lengths_ref[...], 0)
    limit = 1 + jnp.sum(own, axis=1, keepdims=True)
    width = visible_ref.shape[1]
    lane = lax.broadcasted_iota(jnp.int32, (1, width), 1)
    side = lane % 2
    source = partner((lane // 2) % (width // 4), wide_rows)
    first = (source * 2 + lane // (width // 2)) * 3
    visible_ref[:1] = (first + side < limit).astype(jnp.int32)
    visible_ref[1:] = (first + 2 < limit).astype(jnp.int32)


def attend_kernel(visible_ref, query_ref, keys_ref, out_ref):
    heads = out_ref.shape[0]
    keys = keys_ref[...].reshape(2 * keys_ref.shape[0], keys_ref.shape[2])
    width = keys.shape[0]
    half = LATENT_WIDTH // 2
    scores = lax.dot_general(query_ref[...], keys, NT, preferred_element_type=jnp.float32) * score_scale
    lane = lax.broadcasted_iota(jnp.int32, (1, width), 1)
    side = lane % 2
    whole = scores[:heads]
    part = jnp.where(side == 0, scores[heads : 2 * heads], scores[2 * heads :])
    joined = part + jnp.where(side == 0, pltpu.roll(part, width - 1, 1), pltpu.roll(part, 1, 1))
    whole = jnp.where(visible_ref[:1] > 0, whole, floor_value)
    joined = jnp.where(visible_ref[1:] > 0, joined, floor_value)
    highest = jnp.max(jnp.maximum(whole, joined), axis=1, keepdims=True)
    whole = jnp.exp(whole - highest)
    joined = jnp.exp(joined - highest)
    even = jnp.where(side == 0, joined, 0.0)
    odd = joined - even
    weight_sum = jnp.sum(whole + even, axis=1, keepdims=True)
    latent = lax.dot_general(
        whole.astype(keys.dtype), keys[:, :LATENT_WIDTH], NN, preferred_element_type=jnp.float32
    )
    halves = lax.dot_general(
        jnp.concatenate([even, odd], axis=0).astype(keys.dtype),
        keys[:, LATENT_WIDTH : LATENT_WIDTH + half],
        NN,
        preferred_element_type=jnp.float32,
    )
    latent = latent + jnp.concatenate([halves[:heads], halves[heads:]], axis=1)
    out_ref[...] = (latent / weight_sum).astype(out_ref.dtype)


def shards(cache, lengths, slots, query):
    wide_count = lax.axis_size("wide")
    rows = wide_count // COLUMNS
    count = slots.shape[0]
    channels = cache.shape[2]
    rotary = channels - LATENT_WIDTH
    heads = query.shape[2]
    packed_width = LATENT_WIDTH + LATENT_WIDTH // 2 + 2 * rotary
    slot_row = slots.reshape(1, count)
    vmem = pl.BlockSpec(memory_space=pltpu.VMEM)
    hbm = pl.BlockSpec(memory_space=pltpu.HBM)

    def held(a):
        return pltpu.with_memory_space_constraint(a, pltpu.HBM)

    packed, stacked, visible = pl.pallas_call(
        lambda *refs: pack_kernel(rows, *refs),
        out_shape=(
            jax.ShapeDtypeStruct((count, 2, packed_width), cache.dtype),
            jax.ShapeDtypeStruct((3 * heads, packed_width), query.dtype),
            jax.ShapeDtypeStruct((2, 4 * count), jnp.int32),
        ),
        in_specs=[hbm, hbm, hbm, hbm],
        out_specs=(vmem, vmem, vmem),
        scratch_shapes=[
            pltpu.VMEM((1, count), jnp.int32),
            pltpu.VMEM((1, count), jnp.int32),
            pltpu.VMEM((heads, channels), query.dtype),
            pltpu.VMEM((cache.shape[1], channels, count), cache.dtype),
            pltpu.SemaphoreType.DMA((4,)),
        ],
        compiler_params=pltpu.CompilerParams(vmem_limit_bytes=VMEM_BYTES),
        name="pack",
    )(
        held(slot_row),
        held(lengths.reshape(1, count)),
        held(query.reshape(heads, channels)),
        held(jnp.transpose(cache, (1, 2, 0))),
    )
    order = [partner(place, rows) for place in range(wide_count)]
    received = lax.all_to_all(
        packed, "wide", 0, 0, tiled=True, axis_index_groups=[order]
    )
    keys = lax.all_gather(received, "narrow", axis=0, tiled=True)
    attended = pl.pallas_call(
        attend_kernel,
        out_shape=jax.ShapeDtypeStruct((heads, LATENT_WIDTH), jnp.bfloat16),
        in_specs=[vmem, vmem, vmem],
        out_specs=vmem,
        compiler_params=pltpu.CompilerParams(vmem_limit_bytes=VMEM_BYTES),
        name="attend",
    )(visible, stacked, keys)
    return attended.reshape(1, 1, heads, LATENT_WIDTH)


def solution(mesh):
    return jax.shard_map(
        shards,
        mesh=mesh,
        in_specs=(
            P("grp", ("wide", "narrow"), None),
            P("grp"),
            P("grp"),
            P(("grp", "wide"), None, "narrow", None),
        ),
        out_specs=P(("grp", "wide"), None, "narrow", None),
        check_vma=False,
    )
```

```python
import jax
import jax.numpy as jnp
from jax import lax
from jax.experimental import pallas as pl
from jax.experimental.pallas import tpu as pltpu
from jax.sharding import PartitionSpec as P

LATENT_WIDTH = 512
COLUMNS = 4
VMEM_BYTES = 8 << 20

score_scale = 0.0721687836
floor_value = -1e30

NT = (((1,), (1,)), ((), ()))
NN = (((1,), (0,)), ((), ()))


def partner(place, rows):
    step = place // COLUMNS
    run, turn = step % 4, step // 4
    row = turn + (run % 2) * (rows // 2) + (run // 2) * (rows // 4)
    row = row + (run // 3) * (rows // 4 - 1 - 2 * turn)
    return (place % COLUMNS) * rows + row


def place_of(wide, rows):
    column, row = wide // rows, wide % rows
    quarter, turn = row // (rows // 4), row % (rows // 4)
    run = quarter % 2 * 2 + quarter // 2
    turn = turn + (quarter // 3) * (rows // 4 - 1 - 2 * turn)
    return (turn * 4 + run) * COLUMNS + column


def pack_kernel(
    rows,
    slots_hbm,
    lengths_hbm,
    query_hbm,
    cache_hbm,
    packed_ref,
    stacked_ref,
    limit_ref,
    slots_ref,
    lengths_ref,
    query_ref,
    cache_ref,
    arrived,
):
    sources = (slots_hbm, query_hbm, lengths_hbm, cache_hbm)
    places = (slots_ref, query_ref, lengths_ref, cache_ref)
    copies = [pltpu.make_async_copy(a, b, arrived.at[i]) for i, (a, b) in enumerate(zip(sources, places))]
    for copy in copies:
        copy.start()
    count = slots_ref.shape[1]
    rotary = cache_ref.shape[1] - LATENT_WIDTH
    half, half_rotary = LATENT_WIDTH // 2, rotary // 2
    copies[0].wait()
    places_of = place_of(slots_ref[...], rows)
    lane_key = jnp.concatenate([2 * places_of, 2 * places_of + 1], axis=1)
    chosen = lane_key == lax.broadcasted_iota(jnp.int32, (2 * count, 2 * count), 0)
    select = jnp.where(chosen, 1.0, 0.0).astype(cache_ref.dtype)
    copies[1].wait()
    copies[2].wait()
    stack_queries(slots_ref, lengths_ref, query_ref, stacked_ref, limit_ref)
    copies[3].wait()
    parts = []
    for h in range(2):
        parts.append(
            jnp.concatenate(
                [
                    cache_ref[h, :LATENT_WIDTH, :],
                    cache_ref[2, half * h : half * (h + 1), :],
                    cache_ref[h, LATENT_WIDTH:, :],
                    cache_ref[2, LATENT_WIDTH + half_rotary * h : LATENT_WIDTH + half_rotary * (h + 1), :],
                    jnp.zeros((half_rotary, count), cache_ref.dtype),
                ],
                axis=0,
            )
        )
    table = jnp.concatenate(parts, axis=1)
    packed = lax.dot_general(select, table, NT, preferred_element_type=jnp.float32).astype(packed_ref.dtype)
    packed_ref[...] = packed.reshape(packed_ref.shape)


def stack_queries(slots_ref, lengths_ref, query_ref, stacked_ref, limit_ref):
    heads = query_ref.shape[0]
    rotary = query_ref.shape[1] - LATENT_WIDTH
    half, half_rotary = LATENT_WIDTH // 2, rotary // 2
    latent = query_ref[:, :LATENT_WIDTH]
    turned = query_ref[:, LATENT_WIDTH:].astype(jnp.float32)
    turned = jnp.concatenate([turned, jnp.zeros_like(turned)], axis=1)
    lane = lax.broadcasted_iota(jnp.int32, (1, 2 * rotary), 1)
    shared = (lane >= rotary) & (lane < rotary + half_rotary)

    def blank(n):
        return jnp.zeros((heads, n), latent.dtype)

    stacked_ref[:heads] = jnp.concatenate([latent, blank(half), turned.astype(latent.dtype)], axis=1)
    for h in range(2):
        moved = jnp.where(shared, pltpu.roll(turned, rotary - half_rotary * h, 1), 0.0)
        part = latent[:, half * h : half * (h + 1)]
        stacked_ref[heads * (h + 1) : heads * (h + 2)] = jnp.concatenate(
            [blank(LATENT_WIDTH), part, moved.astype(latent.dtype)], axis=1
        )
    own = jnp.where(slots_ref[...] == lax.axis_index("wide"), lengths_ref[...], 0)
    limit_ref[...] = jnp.broadcast_to(1 + jnp.sum(own, axis=1, keepdims=True), limit_ref.shape)


def attend_kernel(rows, limit_ref, query_ref, keys_ref, out_ref):
    heads = out_ref.shape[0]
    keys = keys_ref[...].reshape(2 * keys_ref.shape[0], keys_ref.shape[2])
    width = keys.shape[0]
    half = LATENT_WIDTH // 2
    limit = limit_ref[:, :1]
    scores = lax.dot_general(query_ref[...], keys, NT, preferred_element_type=jnp.float32) * score_scale
    lane = lax.broadcasted_iota(jnp.int32, (1, width), 1)
    side = lane % 2
    place = (lane // 2) % (width // 4)
    source = partner(place, rows)
    first = (source * 2 + lane // (width // 2)) * 3
    whole = scores[:heads]
    part = jnp.where(side == 0, scores[heads : 2 * heads], scores[2 * heads :])
    joined = part + jnp.where(side == 0, pltpu.roll(part, width - 1, 1), pltpu.roll(part, 1, 1))
    whole = jnp.where(first + side < limit, whole, floor_value)
    joined = jnp.where(first + 2 < limit, joined, floor_value)
    highest = jnp.max(jnp.maximum(whole, joined), axis=1, keepdims=True)
    whole = jnp.exp(whole - highest)
    joined = jnp.exp(joined - highest)
    even = jnp.where(side == 0, joined, 0.0)
    odd = joined - even
    weight_sum = jnp.sum(whole + even, axis=1, keepdims=True)
    latent = lax.dot_general(
        whole.astype(keys.dtype), keys[:, :LATENT_WIDTH], NN, preferred_element_type=jnp.float32
    )
    halves = lax.dot_general(
        jnp.concatenate([even, odd], axis=0).astype(keys.dtype),
        keys[:, LATENT_WIDTH : LATENT_WIDTH + half],
        NN,
        preferred_element_type=jnp.float32,
    )
    latent = latent + jnp.concatenate([halves[:heads], halves[heads:]], axis=1)
    out_ref[...] = (latent * (1.0 / weight_sum)).astype(out_ref.dtype)


def shards(cache, lengths, slots, query):
    wide_count = lax.axis_size("wide")
    rows = wide_count // COLUMNS
    count = slots.shape[0]
    channels = cache.shape[2]
    rotary = channels - LATENT_WIDTH
    heads = query.shape[2]
    packed_width = LATENT_WIDTH + LATENT_WIDTH // 2 + 2 * rotary
    slot_row = slots.reshape(1, count)
    vmem = pl.BlockSpec(memory_space=pltpu.VMEM)
    hbm = pl.BlockSpec(memory_space=pltpu.HBM)

    def held(a):
        return pltpu.with_memory_space_constraint(a, pltpu.HBM)

    packed, stacked, limit = pl.pallas_call(
        lambda *refs: pack_kernel(rows, *refs),
        out_shape=(
            jax.ShapeDtypeStruct((count, 2, packed_width), cache.dtype),
            jax.ShapeDtypeStruct((3 * heads, packed_width), query.dtype),
            jax.ShapeDtypeStruct((1, count), jnp.int32),
        ),
        in_specs=[hbm, hbm, hbm, hbm],
        out_specs=(vmem, vmem, vmem),
        scratch_shapes=[
            pltpu.VMEM((1, count), jnp.int32),
            pltpu.VMEM((1, count), jnp.int32),
            pltpu.VMEM((heads, channels), query.dtype),
            pltpu.VMEM((cache.shape[1], channels, count), cache.dtype),
            pltpu.SemaphoreType.DMA((4,)),
        ],
        compiler_params=pltpu.CompilerParams(vmem_limit_bytes=VMEM_BYTES),
        name="pack",
    )(
        held(slot_row),
        held(lengths.reshape(1, count)),
        held(query.reshape(heads, channels)),
        held(jnp.transpose(cache, (1, 2, 0))),
    )
    order = [partner(place, rows) for place in range(wide_count)]
    received = lax.all_to_all(
        packed, "wide", 0, 0, tiled=True, axis_index_groups=[order]
    )
    keys = lax.all_gather(received, "narrow", axis=0, tiled=True)
    attended = pl.pallas_call(
        lambda *refs: attend_kernel(rows, *refs),
        out_shape=jax.ShapeDtypeStruct((heads, LATENT_WIDTH), jnp.bfloat16),
        in_specs=[vmem, vmem, vmem],
        out_specs=vmem,
        compiler_params=pltpu.CompilerParams(vmem_limit_bytes=VMEM_BYTES),
        name="attend",
    )(limit, stacked, keys)
    return attended.reshape(1, 1, heads, LATENT_WIDTH)


def solution(mesh):
    return jax.shard_map(
        shards,
        mesh=mesh,
        in_specs=(
            P("grp", ("wide", "narrow"), None),
            P("grp"),
            P("grp"),
            P(("grp", "wide"), None, "narrow", None),
        ),
        out_specs=P(("grp", "wide"), None, "narrow", None),
        check_vma=False,
    )
```
